256 devices in a mesh: items: 4 (over x), users: 64 (over z, y, core).
Axes of the slice: x: 4, y: 4, z: 8, core: 2. Of those that a mesh axis runs over, the one named last changes fastest.
Arguments:
- capsules: bfloat16 [4096, 8, 128], P('users'), may hold values from -6 to 6
- bank: bfloat16 [262144, 128], P(('items', 'users')), may hold values from -0.5 to 0.5
Outputs:
- relative: float32 [4096, 256], P('users', 'items')
- peak: float32 [4096], P('users')
The draws below stay inside these ranges and needn't reach their ends.
All inputs are finite; a program needn't handle non-finite values.
Results may differ from the reference program's by a relative error of at most 0.0003.
Values may be sent and summed in bfloat16 or wider, within the bound.
A program may use at most 64 MiB of HBM per device.

```python
import jax
import jax.numpy as jnp
from jax import lax

E = 128
K = 8
BLOCK = 1024
USERS = 4096
NB = 256
NITEMS = 262144


def block_levels(key, shape, split, least, largest):
    gain, own = 1.0, jax.random.fold_in(key, 6)
    for axis_at, shards_of in split:
        steps = jnp.exp(jax.random.uniform(jax.random.fold_in(own, axis_at), (shards_of,), jnp.float32, least / len(split), largest / len(split)))
        gain = gain * jnp.repeat(steps, shape[axis_at] // shards_of).reshape([-1 if axis == axis_at else 1 for axis in range(len(shape))])
    return gain


def normal_values(key, shape, scale, limit, split=(), kind=jnp.bfloat16):
    array = scale * jax.random.normal(key, shape, jnp.float32)
    if split:
        array = array * block_levels(key, shape, split, -0.22, 0.18)
    return jnp.clip(array, -limit, limit).astype(kind)


def setup_inputs(seed: int = 0) -> dict:
    streams_of = jax.random.split(jax.random.key(seed), 3)
    capsules = normal_values(streams_of[0], (USERS, K, E), 1.0, 6.0, ((0, 64),))
    bank = normal_values(streams_of[1], (NITEMS, E), E ** -0.5, 0.5, ((0, 256),))
    return {"capsules": capsules, "bank": bank}


def reference(capsules, bank):
    flat = capsules.reshape(USERS * K, E)
    blocks = bank.reshape(NB, BLOCK, E)

    def one_block(rows):
        score = jnp.dot(flat, rows.T, preferred_element_type=jnp.float32)
        return jnp.max(score.reshape(USERS, K * BLOCK), axis=1)

    block_peak = lax.map(one_block, blocks).T
    peak = jnp.max(block_peak, axis=1)
    return block_peak - peak[:, None], peak
```

```python
import jax
import jax.numpy as jnp
from jax import lax
from jax.experimental import pallas as pl
from jax.experimental.pallas import tpu as pltpu
from jax.sharding import PartitionSpec as P

K = 8
E = 128
BLOCK = 1024
USERS = 64
NX, NZ, NY = 4, 8, 4
COLS = USERS * K
TILE = COLS // 2
HALF = BLOCK // 2
ROWS = 256
MESH = pl.DeviceIdType.MESH

DZ = (0, -1, -2, -3, 1, 2, 3, 4)
DY = (0, -1, 1, 2)


def units_of(groups, blocks):
    return [("u", g, b, h) for g in groups for b, h in blocks]


def full(*slots):
    return [(b, h) for b in slots for h in (0, 1)]


def half(h, *slots):
    return [(b, h) for b in slots]


def wait_c(*pieces):
    return [("c", s, t) for s, t in pieces]


def wait_b(*pieces):
    return [("b", s, h) for s, h in pieces]


def program():
    order = []
    order += units_of([0], full(0))
    order += wait_b((4, 0), (4, 1))
    order += units_of([0], full(4))
    order += wait_c((1, 0), (4, 1), (1, 1))
    order += units_of([1], full(0, 4))
    order += wait_c((4, 0)) + wait_b((1, 0), (2, 0))
    order += units_of([4], full(0, 4))
    order += units_of([0, 1, 4], half(0, 1, 2))
    order += wait_b((5, 0), (6, 0)) + wait_c((2, 0), (5, 1))
    order += units_of([0, 1, 4], half(0, 5, 6))
    order += wait_c((2, 1), (5, 0)) + wait_b((1, 1), (2, 1))
    order += units_of([2, 5], full(0, 4) + half(0, 1, 2, 5, 6))
    order += wait_b((5, 1), (6, 1)) + wait_c((3, 0), (6, 1))
    order += units_of([2, 5], half(1, 1, 2, 5, 6))
    order += wait_c((3, 1), (6, 0)) + wait_b((3, 0), (3, 1))
    order += units_of([3, 6], full(0, 4, 1, 2, 5, 6))
    order += wait_b((7, 0), (7, 1)) + wait_c((7, 0), (7, 1)) + [("ready1",)]
    order += units_of([7], full(0, 4, 1, 2))
    order += [("ready2",)]
    order += units_of([7], full(5, 6))
    order += [("ready3",)]
    order += units_of([7, 3, 6, 2, 5], full(3, 7))
    order += units_of([1, 4, 0], half(1, 1, 2, 5, 6) + full(3, 7))
    assert len({o for o in order if o[0] == "u"}) == 128
    return order


def widened(value):
    return jnp.concatenate([value, jnp.zeros_like(value)], axis=1)


def kernel(
    caps_hbm, bank_hbm, out_ref, peak_ref,
    caps, bank, peaks, rows, tiles, table, turned,
    local_sem, cap_sem, bank_sem, tile_sem, cap_send, bank_send, tile_send, ready_a, ready_b,
):
    x = lax.axis_index("items")
    u = lax.axis_index("users")
    z = lax.div(u, 2 * NY)
    y = lax.rem(lax.div(u, 2), NY)
    core = lax.rem(u, 2)
    xs = [lax.rem(x + dx, NX) for dx in range(NX)]
    ys = [lax.rem(y + dy, NY) for dy in range(NY)]
    zs = [lax.rem(z + dz, NZ) for dz in range(NZ)]
    here = x * NZ + z
    users_at = {}
    for dz in range(NZ):
        users_at[dz, 0, 0] = (zs[dz] * NY + y) * 2 + core
    for dy in range(1, NY):
        users_at[0, dy, 0] = (z * NY + ys[dy]) * 2 + core
    users_at[0, 0, 1] = (z * NY + y) * 2 + 1 - core
    row_of = [2 * ys[DY[b % 4] % NY] + (core if b < 4 else 1 - core) for b in range(8)]

    def device(dx=0, dz=0, dy=0, flip=0):
        return {"items": xs[dx % NX], "users": users_at[dz % NZ, dy % NY, flip]}

    def cap_part(slot, t):
        return caps.at[slot, pl.ds(t * TILE, TILE), :]

    def bank_part(slot, h):
        return bank.at[slot, pl.ds(h * HALF, HALF), :]

    sent = []

    def send(src, dst, send_sem, recv_sem, to):
        copy = pltpu.make_async_remote_copy(
            src_ref=src, dst_ref=dst, send_sem=send_sem, recv_sem=recv_sem, device_id=to, device_id_type=MESH
        )
        copy.start()
        sent.append(copy)

    counts = {"c": 0, "b": 0, "t": 0}

    def send_cap(slot, t, to_slot, dz):
        n = counts["c"]
        counts["c"] += 1
        send(cap_part(slot, t), cap_part(to_slot, t), cap_send.at[n], cap_sem.at[to_slot, t], device(dz=dz))

    def send_bank(slot, h, to_slot, **to):
        n = counts["b"]
        counts["b"] += 1
        send(bank_part(slot, h), bank_part(to_slot, h), bank_send.at[n], bank_sem.at[to_slot, h], device(**to))

    def forward_cap(slot, t):
        if slot in (1, 2):
            send_cap(slot, t, slot + 1, 1)
        elif slot == 3 and t == 0:
            send_cap(3, 0, 7, 1)
        elif slot in (4, 5):
            send_cap(slot, t, slot + 1, -1)
        elif slot == 6 and t == 1:
            send_cap(6, 1, 7, -1)

    def forward_bank(slot, h):
        if slot == 1 and h == 0:
            send_bank(1, 0, 3, dy=1)
        if slot == 2 and h == 1:
            send_bank(2, 1, 3, dy=-1)
        if slot < 4:
            send_bank(slot, h, slot + 4, flip=1)

    def arrived(ref, sem):
        pltpu.make_async_copy(ref, ref, sem).wait()

    def body(*accs):
        accs = (accs[:4], accs[4:])
        own = []
        for t in range(2):
            own.append(pltpu.make_async_copy(caps_hbm.at[pl.ds(t * TILE, TILE), :], cap_part(0, t), local_sem.at[t]))
        for h in range(2):
            own.append(pltpu.make_async_copy(bank_hbm.at[pl.ds(h * HALF, HALF), :], bank_part(0, h), local_sem.at[2 + h]))
        for copy in own:
            copy.start()

        barrier = pltpu.get_barrier_semaphore()
        neighbours = [
            device(flip=1), device(dz=1), device(dz=-1), device(dy=1), device(dy=-1), device(dx=1), device(dx=NX - 1),
        ]
        for neighbour in neighbours:
            pl.semaphore_signal(barrier, inc=1, device_id=neighbour, device_id_type=MESH)

        nothing = jnp.zeros((ROWS, 2 * E), jnp.bfloat16)
        for m in range(2):
            pltpu.matmul_acc_lhs(accs[m][3], nothing, load_staged_rhs=0)
        for m in range(2):
            for acc in accs[m]:
                pltpu.matmul_pop(acc)

        pl.semaphore_wait(barrier, len(neighbours))
        for t in range(2):
            own[t].wait()
        send_cap(0, 0, 1, 1)
        send_cap(0, 1, 4, -1)
        send_cap(0, 1, 1, 1)
        send_cap(0, 0, 4, -1)
        for h in range(2):
            own[2 + h].wait()
            send_bank(0, h, 4, flip=1)
            send_bank(0, h, 1, dy=1)
            send_bank(0, h, 2, dy=-1)

        lane = lax.broadcasted_iota(jnp.int32, (8, 128), 1) % K

        def finish(g):
            found = peaks[g].reshape(8, 2, 8, COLS)
            found = jnp.max(jnp.maximum(found[:, 0], found[:, 1]), axis=1)
            for b in range(8):
                rows[pl.ds(row_of[b], 1), :] = found[b : b + 1, :]
            whole = None
            for q in range(4):
                part = rows[:, q * 128 : (q + 1) * 128]
                for shift in (1, 2, 4):
                    part = jnp.maximum(part, pltpu.roll(part, 128 - shift, 1))
                if q:
                    part = pltpu.roll(part, q, 1)
                whole = part if whole is None else jnp.where(lane == q, part, whole)
            tiles[g] = whole
            if g == 0:
                table[here] = whole
            for dx in range(NX):
                if g == 0 and dx == 0:
                    continue
                n = counts["t"]
                counts["t"] += 1
                send(tiles.at[g], table.at[here], tile_send.at[n], tile_sem.at[here], device(dx=dx, dz=DZ[g]))

        order = program()
        units = [o[1:] for o in order if o[0] == "u"]
        state = {"n": 0, "loaded": None}
        pending = []
        partial = [None, None]
        left = [32] * 8

        def pop_one():
            (g, b, h), c, slot = pending.pop(0)
            for m in range(2):
                value = jnp.max(pltpu.matmul_pop(accs[m][slot]).reshape(ROWS // 8, 8, 2 * E), axis=0)
                if c == 0:
                    partial[m] = value
                else:
                    peaks[g, 2 * b + h, :, m * TILE : (m + 1) * TILE] = jnp.maximum(partial[m], value)
            left[g] -= 1
            if left[g] == 0:
                finish(g)

        def push(g):
            for m in range(2):
                pltpu.matmul_push_rhs(
                    widened(caps[g, m * TILE : (m + 1) * TILE, :]), staging_register=0, mxu_index=m, transpose=True
                )

        present = {0}
        at = 0
        for step in order:
            if step[0] == "c":
                _, slot, t = step
                arrived(cap_part(slot, t), cap_sem.at[slot, t])
                forward_cap(slot, t)
                continue
            if step[0] == "b":
                _, slot, h = step
                arrived(bank_part(slot, h), bank_sem.at[slot, h])
                forward_bank(slot, h)
                continue
            if step[0] == "ready1":
                for dx in (1, NX - 1):
                    pl.semaphore_signal(ready_a, inc=1, device_id=device(dx=dx), device_id_type=MESH)
                continue
            if step[0] == "ready2":
                pl.semaphore_wait(ready_a, 2)
                pl.semaphore_signal(ready_b, inc=1, device_id=device(dx=1), device_id_type=MESH)
                continue
            if step[0] == "ready3":
                pl.semaphore_wait(ready_b, 1)
                continue
            g, b, h = step[1:]
            for c in range(HALF // ROWS):
                first = h * HALF + c * ROWS
                lhs = widened(bank[b, first : first + ROWS, :])
                slot = state["n"] % 4
                state["n"] += 1
                fresh = state["loaded"] != g
                if fresh:
                    push(g)
                    state["loaded"] = g
                for m in range(2):
                    pltpu.matmul_acc_lhs(accs[m][slot], lhs, load_staged_rhs=0 if fresh else None)
                pending.append(((g, b, h), c, slot))
                if len(pending) > 2:
                    pop_one()
        while pending:
            pop_one()

        for dz in range(NZ):
            for dx in range(NX):
                if dx or dz:
                    source = xs[dx] * NZ + zs[dz]
                    arrived(table.at[source], tile_sem.at[source])

        best = jnp.max(jnp.max(table[...], axis=0), axis=0, keepdims=True)
        mine = table[pl.ds(x * NZ, NZ)].reshape(NZ * 8, 128)
        both = jnp.concatenate([mine - best, jnp.broadcast_to(best, (128 - NZ * 8, 128))], axis=0)
        turned[...] = both.T
        by_user = jnp.concatenate([turned[pl.ds(q, USERS // 4, stride=K), :] for q in range(4)], axis=0)
        out_ref[...] = by_user[:, : NZ * 8]
        square = jnp.concatenate([by_user, by_user], axis=0).T
        peak_ref[...] = square[NZ * 8 : NZ * 8 + 8, :]

        for copy in sent:
            copy.wait_send()

    pl.run_scoped(
        body,
        *[pltpu.ACC(0)((ROWS, 2 * E), jnp.float32)] * 4,
        *[pltpu.ACC(1)((ROWS, 2 * E), jnp.float32)] * 4,
    )


def per_device(capsules, bank):
    dma = pltpu.SemaphoreType.DMA
    relative, peak = pl.pallas_call(
        kernel,
        out_shape=(
            jax.ShapeDtypeStruct((USERS, NZ * 8), jnp.float32),
            jax.ShapeDtypeStruct((8, 128), jnp.float32),
        ),
        in_specs=[pl.BlockSpec(memory_space=pltpu.HBM)] * 2,
        out_specs=(pl.BlockSpec(memory_space=pltpu.VMEM),) * 2,
        scratch_shapes=[
            pltpu.VMEM((8, COLS, E), jnp.bfloat16),
            pltpu.VMEM((8, BLOCK, E), jnp.bfloat16),
            pltpu.VMEM((8, 16, 8, COLS), jnp.float32),
            pltpu.VMEM((8, COLS), jnp.float32),
            pltpu.VMEM((8, 8, 128), jnp.float32),
            pltpu.VMEM((NX * NZ, 8, 128), jnp.float32),
            pltpu.VMEM((128, 128), jnp.float32),
            dma((4,)), dma((8, 2)), dma((8, 2)), dma((NX * NZ,)),
            dma((14,)), dma((14,)), dma((31,)),
            pltpu.SemaphoreType.REGULAR, pltpu.SemaphoreType.REGULAR,
        ],
        compiler_params=pltpu.CompilerParams(
            collective_id=0, has_side_effects=True, vmem_limit_bytes=62 << 20
        ),
        name="peaks",
    )(capsules.reshape(COLS, E), bank)
    return relative, peak[0, :USERS]


def solution(mesh):
    return jax.shard_map(
        per_device,
        mesh=mesh,
        in_specs=(P("users", None, None), P(("items", "users"), None)),
        out_specs=(P("users", "items"), P("users")),
        check_vma=False,
    )
```

```python
import jax
import jax.numpy as jnp
from jax import lax
from jax.experimental import pallas as pl
from jax.experimental.pallas import tpu as pltpu
from jax.sharding import PartitionSpec as P

K = 8
E = 128
BLOCK = 1024
USERS = 64
NX, NZ, NY = 4, 8, 4
COLS = USERS * K
TILE = COLS // 2
HALF = BLOCK // 2
ROWS = 256
MESH = pl.DeviceIdType.MESH

DZ = (0, -1, -2, -3, 1, 2, 3, 4)
DY = (0, -1, 1, 2)


def units_of(pairs, blocks):
    return [("u", *pair, b, h) for pair in pairs for b, h in blocks]


def full(*slots):
    return [(b, h) for b in slots for h in (0, 1)]


def half(h, *slots):
    return [(b, h) for b in slots]


def wait_c(*pieces):
    return [("c", s, t) for s, t in pieces]


def wait_b(*pieces):
    return [("b", s, h) for s, h in pieces]


def program():
    own, low, high, opposite = (0, 0), [(1, 4), (2, 5), (3, 6)], [(4, 1), (5, 2), (6, 3)], (7, 7)
    order = []
    order += units_of([own], full(0))
    order += wait_b((4, 0), (4, 1))
    order += units_of([own], full(4))
    order += wait_c((1, 0), (4, 1))
    order += units_of([low[0]], full(0, 4))
    order += wait_c((1, 1), (4, 0))
    order += units_of([high[0]], full(0, 4))
    order += wait_b((1, 0), (2, 0))
    order += units_of([own, low[0], high[0]], half(0, 1, 2))
    order += wait_b((5, 0), (6, 0))
    order += units_of([high[0], low[0]], half(0, 5, 6))
    order += wait_c((2, 0), (5, 1))
    order += units_of([own], half(0, 5, 6))
    order += units_of([low[1]], full(0, 4) + half(0, 1, 2))
    order += wait_c((2, 1), (5, 0)) + wait_b((1, 1), (2, 1))
    order += units_of([low[1]], half(0, 5, 6))
    order += units_of([high[1]], full(0, 4) + half(0, 1, 2, 5, 6))
    order += wait_b((5, 1), (6, 1))
    order += units_of([high[1], low[1]], half(1, 1, 2, 5, 6))
    order += wait_c((3, 0), (6, 1))
    order += units_of([low[0], high[0]], half(1, 1, 2, 5, 6))
    order += units_of([low[2]], full(0, 4))
    order += wait_c((3, 1), (6, 0)) + wait_b((3, 0), (3, 1))
    order += units_of([low[2]], full(1, 2, 5, 6))
    order += wait_b((7, 0), (7, 1))
    order += units_of([high[2]], full(0, 4))
    order += wait_c((7, 0), (7, 1)) + [("ready1",)]
    order += units_of([high[2]], full(1, 2, 5, 6))
    order += units_of([opposite], full(0, 4))
    order += [("ready2",)]
    order += units_of([opposite], full(1, 2, 5, 6))
    order += [("ready3",)]
    order += units_of([(g, g) for g in (4, 5, 6, 7, 3, 2, 1)], full(3, 7))
    order += units_of([own], half(1, 1, 2, 5, 6) + full(3, 7))
    assert len({o for o in order if o[0] == "u"}) == 128
    return order


def widened(value):
    return jnp.concatenate([value, jnp.zeros_like(value)], axis=1)


def kernel(
    caps_hbm, bank_hbm, table,
    caps, bank, peaks, rows, tiles,
    local_sem, cap_sem, bank_sem, tile_sem, send_sem, ready_a, ready_b,
):
    x = lax.axis_index("items")
    u = lax.axis_index("users")
    z = lax.div(u, 2 * NY)
    y = lax.rem(lax.div(u, 2), NY)
    core = lax.rem(u, 2)
    xs = [lax.rem(x + dx, NX) for dx in range(NX)]
    ys = [lax.rem(y + dy, NY) for dy in range(NY)]
    zs = [lax.rem(z + dz, NZ) for dz in range(NZ)]
    here = x * NZ + z
    users_at = {}
    for dz in range(NZ):
        users_at[dz, 0, 0] = (zs[dz] * NY + y) * 2 + core
    for dy in range(1, NY):
        users_at[0, dy, 0] = (z * NY + ys[dy]) * 2 + core
    users_at[0, 0, 1] = (z * NY + y) * 2 + 1 - core
    row_of = [2 * ys[DY[b % 4] % NY] + (core if b < 4 else 1 - core) for b in range(8)]

    def device(dx=0, dz=0, dy=0, flip=0):
        return {"items": xs[dx % NX], "users": users_at[dz % NZ, dy % NY, flip]}

    def cap_part(slot, t):
        return caps.at[slot, pl.ds(t * TILE, TILE), :]

    def bank_part(slot, h):
        return bank.at[slot, pl.ds(h * HALF, HALF), :]

    def send(src, dst, send_sem, recv_sem, to):
        pltpu.make_async_remote_copy(
            src_ref=src, dst_ref=dst, send_sem=send_sem, recv_sem=recv_sem, device_id=to, device_id_type=MESH
        ).start()

    def send_cap(slot, t, to_slot, dz):
        send(cap_part(slot, t), cap_part(to_slot, t), send_sem.at[0], cap_sem.at[to_slot, t], device(dz=dz))

    def send_bank(slot, h, to_slot, **to):
        send(bank_part(slot, h), bank_part(to_slot, h), send_sem.at[1], bank_sem.at[to_slot, h], device(**to))

    def forward_cap(slot, t):
        if slot in (1, 2):
            send_cap(slot, t, slot + 1, 1)
        elif slot == 3 and t == 0:
            send_cap(3, 0, 7, 1)
        elif slot in (4, 5):
            send_cap(slot, t, slot + 1, -1)
        elif slot == 6 and t == 1:
            send_cap(6, 1, 7, -1)

    def forward_bank(slot, h):
        if slot == 1 and h == 0:
            send_bank(1, 0, 3, dy=1)
        if slot == 2 and h == 1:
            send_bank(2, 1, 3, dy=-1)
        if slot < 4:
            send_bank(slot, h, slot + 4, flip=1)

    def arrived(ref, sem):
        pltpu.make_async_copy(ref, ref, sem).wait()

    def body(*accs):
        accs = (accs[:4], accs[4:])
        own = []
        for t in range(2):
            own.append(pltpu.make_async_copy(caps_hbm.at[pl.ds(t * TILE, TILE), :], cap_part(0, t), local_sem.at[t]))
        for h in range(2):
            own.append(pltpu.make_async_copy(bank_hbm.at[pl.ds(h * HALF, HALF), :], bank_part(0, h), local_sem.at[2 + h]))
        for copy in own:
            copy.start()

        barrier = pltpu.get_barrier_semaphore()
        neighbours = [
            device(flip=1), device(dz=1), device(dz=-1), device(dy=1), device(dy=-1), device(dx=1), device(dx=NX - 1),
        ]
        for neighbour in neighbours:
            pl.semaphore_signal(barrier, inc=1, device_id=neighbour, device_id_type=MESH)

        nothing = jnp.zeros((ROWS, 2 * E), jnp.bfloat16)
        for m in range(2):
            pltpu.matmul_acc_lhs(accs[m][3], nothing, load_staged_rhs=0)
        for m in range(2):
            for acc in accs[m]:
                pltpu.matmul_pop(acc)

        pl.semaphore_wait(barrier, len(neighbours))
        for t in range(2):
            own[t].wait()
        send_cap(0, 0, 1, 1)
        send_cap(0, 1, 4, -1)
        send_cap(0, 1, 1, 1)
        send_cap(0, 0, 4, -1)
        for h in range(2):
            own[2 + h].wait()
            send_bank(0, h, 4, flip=1)
            send_bank(0, h, 1, dy=1)
            send_bank(0, h, 2, dy=-1)

        lane = lax.broadcasted_iota(jnp.int32, (8, 128), 1) % K

        def finish(g):
            whole = None
            for q in range(4):
                part = rows[g, :, q * 128 : (q + 1) * 128]
                for shift in (1, 2, 4):
                    part = jnp.maximum(part, pltpu.roll(part, 128 - shift, 1))
                if q:
                    part = pltpu.roll(part, q, 1)
                whole = part if whole is None else jnp.where(lane == q, part, whole)
            tiles[g] = whole
            if g == 0:
                table[here] = whole

        def deliver(g):
            for dx in range(NX):
                if g == 0 and dx == 0:
                    continue
                send(tiles.at[g], table.at[here], send_sem.at[2], tile_sem, device(dx=dx, dz=DZ[g]))

        order = program()
        pending = []
        loaded = [None, None]
        partial = [None, None]
        left = [64] * 8
        begun = set()
        ready = []
        chunks = 0

        def pop_one():
            groups, b, c, slot = pending.pop(0)
            for m in range(2):
                g = groups[m]
                value = jnp.max(pltpu.matmul_pop(accs[m][slot]).reshape(ROWS // 8, 8, 2 * E), axis=0)
                left[g] -= 1
                if c == 0:
                    partial[m] = value
                    continue
                value = jnp.maximum(partial[m], value)
                columns = slice(m * TILE, (m + 1) * TILE)
                if (m, g, b) not in begun:
                    begun.add((m, g, b))
                    peaks[g, b, :, columns] = value
                else:
                    value = jnp.maximum(peaks[g, b, :, columns], value)
                    rows[g, pl.ds(row_of[b], 1), columns] = jnp.max(value, axis=0, keepdims=True)
            for g in sorted(set(groups)):
                if left[g] == 0:
                    finish(g)
                    ready.append([2, g])

        def push(m, g):
            pltpu.matmul_push_rhs(
                widened(caps[g, m * TILE : (m + 1) * TILE, :]), staging_register=0, mxu_index=m, transpose=True
            )

        for step in order:
            if step[0] == "c":
                _, slot, t = step
                arrived(cap_part(slot, t), cap_sem.at[slot, t])
                forward_cap(slot, t)
                continue
            if step[0] == "b":
                _, slot, h = step
                arrived(bank_part(slot, h), bank_sem.at[slot, h])
                forward_bank(slot, h)
                continue
            if step[0] == "ready1":
                for dx in (1, NX - 1):
                    pl.semaphore_signal(ready_a, inc=1, device_id=device(dx=dx), device_id_type=MESH)
                continue
            if step[0] == "ready2":
                pl.semaphore_wait(ready_a, 2)
                pl.semaphore_signal(ready_b, inc=1, device_id=device(dx=1), device_id_type=MESH)
                continue
            if step[0] == "ready3":
                pl.semaphore_wait(ready_b, 1)
                continue
            for item in ready:
                item[0] -= 1
            while ready and ready[0][0] < 0:
                deliver(ready.pop(0)[1])
            groups, b, h = step[1:3], step[3], step[4]
            for c in range(HALF // ROWS):
                first = h * HALF + c * ROWS
                lhs = widened(bank[b, first : first + ROWS, :])
                slot = chunks % 4
                chunks += 1
                for m in range(2):
                    fresh = loaded[m] != groups[m]
                    if fresh:
                        push(m, groups[m])
                        loaded[m] = groups[m]
                    pltpu.matmul_acc_lhs(accs[m][slot], lhs, load_staged_rhs=0 if fresh else None)
                pending.append((groups, b, c, slot))
                if len(pending) > 2:
                    pop_one()
        while pending:
            pop_one()
        while ready:
            deliver(ready.pop(0)[1])

        arrived(table.at[pl.ds(0, NX * NZ - 1)], tile_sem)
        arrived(caps.at[pl.ds(0, 7)], send_sem.at[0])
        arrived(bank.at[pl.ds(0, 7)], send_sem.at[1])
        arrived(table.at[pl.ds(0, NX * NZ - 1)], send_sem.at[2])

    pl.run_scoped(
        body,
        *[pltpu.ACC(0)((ROWS, 2 * E), jnp.float32)] * 4,
        *[pltpu.ACC(1)((ROWS, 2 * E), jnp.float32)] * 4,
    )


def ending(table, out_ref, peak_ref, turned):
    x = lax.axis_index("items")
    best = jnp.max(jnp.max(table[...], axis=0), axis=0, keepdims=True)
    mine = table[pl.ds(x * NZ, NZ)].reshape(NZ * 8, 128)
    both = jnp.concatenate([mine - best, jnp.broadcast_to(best, (128 - NZ * 8, 128))], axis=0)
    turned[...] = both.T
    by_user = jnp.concatenate([turned[pl.ds(q, USERS // 4, stride=K), :] for q in range(4)], axis=0)
    out_ref[...] = by_user[:, : NZ * 8]
    square = jnp.concatenate([by_user, by_user], axis=0).T
    peak_ref[...] = square[NZ * 8, :USERS]


def per_device(capsules, bank):
    dma = pltpu.SemaphoreType.DMA
    vmem = pl.BlockSpec(memory_space=pltpu.VMEM)
    table = pl.pallas_call(
        kernel,
        out_shape=jax.ShapeDtypeStruct((NX * NZ, 8, 128), jnp.float32),
        in_specs=[pl.BlockSpec(memory_space=pltpu.HBM)] * 2,
        out_specs=vmem,
        scratch_shapes=[
            pltpu.VMEM((8, COLS, E), jnp.bfloat16),
            pltpu.VMEM((8, BLOCK, E), jnp.bfloat16),
            pltpu.VMEM((8, 8, 8, COLS), jnp.float32),
            pltpu.VMEM((8, 8, COLS), jnp.float32),
            pltpu.VMEM((8, 8, 128), jnp.float32),
            dma((4,)), dma((8, 2)), dma((8, 2)), dma, dma((3,)),
            pltpu.SemaphoreType.REGULAR, pltpu.SemaphoreType.REGULAR,
        ],
        compiler_params=pltpu.CompilerParams(
            collective_id=0, has_side_effects=True, vmem_limit_bytes=40 << 20
        ),
        name="peaks",
    )(
        pltpu.with_memory_space_constraint(capsules.reshape(COLS, E), pltpu.HBM),
        pltpu.with_memory_space_constraint(bank, pltpu.HBM),
    )
    return pl.pallas_call(
        ending,
        out_shape=(
            jax.ShapeDtypeStruct((USERS, NZ * 8), jnp.float32),
            jax.ShapeDtypeStruct((USERS,), jnp.float32),
        ),
        in_specs=[vmem],
        out_specs=(vmem, vmem),
        scratch_shapes=[pltpu.VMEM((128, 128), jnp.float32)],
        compiler_params=pltpu.CompilerParams(vmem_limit_bytes=4 << 20),
        name="ending",
    )(table)


def solution(mesh):
    return jax.shard_map(
        per_device,
        mesh=mesh,
        in_specs=(P("users", None, None), P(("items", "users"), None)),
        out_specs=(P("users", "items"), P("users")),
        check_vma=False,
    )
```

```python
import jax
import jax.numpy as jnp
from jax import lax
from jax.experimental import pallas as pl
from jax.experimental.pallas import tpu as pltpu
from jax.sharding import PartitionSpec as P

K = 8
E = 128
BLOCK = 1024
USERS = 64
NX, NZ, NY = 4, 8, 4
COLS = USERS * K
TILE = COLS // 2
HALF = BLOCK // 2
ROWS = 256
MESH = pl.DeviceIdType.MESH

DZ = (0, -1, -2, -3, 1, 2, 3, 4)
DY = (0, -1, 1, 2)


def units_of(pairs, blocks):
    return [("u", *pair, b, h) for pair in pairs for b, h in blocks]


def full(*slots):
    return [(b, h) for b in slots for h in (0, 1)]


def half(h, *slots):
    return [(b, h) for b in slots]


def wait_c(*pieces):
    return [("c", s, t) for s, t in pieces]


def wait_b(*pieces):
    return [("b", s, h) for s, h in pieces]


def program():
    own, low, high, opposite = (0, 0), [(1, 4), (2, 5), (3, 6)], [(4, 1), (5, 2), (6, 3)], (7, 7)
    order = []
    order += units_of([own], full(0))
    order += wait_b((4, 0), (4, 1))
    order += units_of([own], full(4))
    order += wait_c((1, 0), (4, 1))
    order += units_of([low[0]], full(0, 4))
    order += wait_c((1, 1), (4, 0))
    order += units_of([high[0]], full(0, 4))
    order += wait_b((1, 0), (2, 0))
    order += units_of([own, low[0], high[0]], half(0, 1, 2))
    order += wait_b((5, 0), (6, 0))
    order += units_of([high[0], low[0]], half(0, 5, 6))
    order += wait_c((2, 0), (5, 1))
    order += units_of([own], half(0, 5, 6))
    order += units_of([low[1]], full(0, 4) + half(0, 1, 2))
    order += wait_c((2, 1), (5, 0)) + wait_b((1, 1), (2, 1))
    order += units_of([low[1]], half(0, 5, 6))
    order += units_of([high[1]], full(0, 4) + half(0, 1, 2, 5, 6))
    order += wait_b((5, 1), (6, 1))
    order += units_of([high[1], low[1], low[0]], half(1, 1, 2, 5, 6))
    order += wait_c((3, 0), (6, 1))
    order += units_of([high[0]], half(1, 1, 2, 5, 6))
    order += wait_b((3, 0), (3, 1))
    order += units_of([low[2]], full(0, 4))
    order += wait_c((3, 1), (6, 0)) + [("ready1",)]
    order += units_of([low[2]], full(1, 2, 5, 6))
    order += wait_b((7, 0), (7, 1))
    order += units_of([high[2]], full(0, 4, 1, 2))
    order += [("ready2",)] + wait_c((7, 0), (7, 1))
    order += units_of([high[2]], full(5, 6))
    order += units_of([opposite], full(0, 4, 1, 2))
    order += [("ready3",)]
    order += units_of([opposite], full(5, 6))
    order += units_of([(g, g) for g in (4, 5, 6, 7, 3, 2, 1)], full(3, 7))
    order += units_of([own], half(1, 1, 2, 5, 6) + full(3, 7))
    assert len({o for o in order if o[0] == "u"}) == 128
    return order


def widened(value):
    return jnp.concatenate([value, jnp.zeros_like(value)], axis=1)


def kernel(
    caps_hbm, bank_hbm, table,
    caps, bank, peaks, rows, tiles,
    local_sem, cap_sem, bank_sem, tile_sem, send_sem, ready_a, ready_b,
):
    x = lax.axis_index("items")
    u = lax.axis_index("users")
    z = lax.div(u, 2 * NY)
    y = lax.rem(lax.div(u, 2), NY)
    core = lax.rem(u, 2)
    xs = [lax.rem(x + dx, NX) for dx in range(NX)]
    ys = [lax.rem(y + dy, NY) for dy in range(NY)]
    zs = [lax.rem(z + dz, NZ) for dz in range(NZ)]
    here = x * NZ + z
    users_at = {}
    for dz in range(NZ):
        users_at[dz, 0, 0] = (zs[dz] * NY + y) * 2 + core
    for dy in range(1, NY):
        users_at[0, dy, 0] = (z * NY + ys[dy]) * 2 + core
    users_at[0, 0, 1] = (z * NY + y) * 2 + 1 - core
    row_of = [2 * ys[DY[b % 4] % NY] + (core if b < 4 else 1 - core) for b in range(8)]

    def device(dx=0, dz=0, dy=0, flip=0):
        return {"items": xs[dx % NX], "users": users_at[dz % NZ, dy % NY, flip]}

    def cap_part(slot, t):
        return caps.at[slot, pl.ds(t * TILE, TILE), :]

    def bank_part(slot, h):
        return bank.at[slot, pl.ds(h * HALF, HALF), :]

    def send(src, dst, send_sem, recv_sem, to):
        pltpu.make_async_remote_copy(
            src_ref=src, dst_ref=dst, send_sem=send_sem, recv_sem=recv_sem, device_id=to, device_id_type=MESH
        ).start()

    def send_cap(slot, t, to_slot, dz):
        send(cap_part(slot, t), cap_part(to_slot, t), send_sem.at[0], cap_sem.at[to_slot, t], device(dz=dz))

    def send_bank(slot, h, to_slot, **to):
        send(bank_part(slot, h), bank_part(to_slot, h), send_sem.at[1], bank_sem.at[to_slot, h], device(**to))

    def forward_cap(slot, t):
        if slot in (1, 2):
            send_cap(slot, t, slot + 1, 1)
        elif slot == 3 and t == 0:
            send_cap(3, 0, 7, 1)
        elif slot in (4, 5):
            send_cap(slot, t, slot + 1, -1)
        elif slot == 6 and t == 1:
            send_cap(6, 1, 7, -1)

    def forward_bank(slot, h):
        if slot == 1 and h == 0:
            send_bank(1, 0, 3, dy=1)
        if slot == 2 and h == 1:
            send_bank(2, 1, 3, dy=-1)
        if slot < 4:
            send_bank(slot, h, slot + 4, flip=1)

    def arrived(ref, sem):
        pltpu.make_async_copy(ref, ref, sem).wait()

    def body(*accs):
        accs = (accs[:4], accs[4:])
        own = []
        for t in range(2):
            own.append(pltpu.make_async_copy(caps_hbm.at[pl.ds(t * TILE, TILE), :], cap_part(0, t), local_sem.at[t]))
        for h in range(2):
            own.append(pltpu.make_async_copy(bank_hbm.at[pl.ds(h * HALF, HALF), :], bank_part(0, h), local_sem.at[2 + h]))
        for copy in own:
            copy.start()

        barrier = pltpu.get_barrier_semaphore()
        neighbours = [
            device(flip=1), device(dz=1), device(dz=-1), device(dy=1), device(dy=-1), device(dx=1), device(dx=NX - 1),
        ]
        for neighbour in neighbours:
            pl.semaphore_signal(barrier, inc=1, device_id=neighbour, device_id_type=MESH)

        nothing = jnp.zeros((ROWS, 2 * E), jnp.bfloat16)
        for m in range(2):
            pltpu.matmul_acc_lhs(accs[m][3], nothing, load_staged_rhs=0)
        for m in range(2):
            for acc in accs[m]:
                pltpu.matmul_pop(acc)

        pl.semaphore_wait(barrier, len(neighbours))
        for t in range(2):
            own[t].wait()
        send_cap(0, 0, 1, 1)
        send_cap(0, 1, 4, -1)
        send_cap(0, 1, 1, 1)
        send_cap(0, 0, 4, -1)
        for h in range(2):
            own[2 + h].wait()
            send_bank(0, h, 4, flip=1)
            send_bank(0, h, 1, dy=1)
            send_bank(0, h, 2, dy=-1)

        lane = lax.broadcasted_iota(jnp.int32, (8, 128), 1) % K

        def finish(g):
            whole = None
            for q in range(4):
                part = rows[g, :, q * 128 : (q + 1) * 128]
                for shift in (1, 2, 4):
                    part = jnp.maximum(part, pltpu.roll(part, 128 - shift, 1))
                if q:
                    part = pltpu.roll(part, q, 1)
                whole = part if whole is None else jnp.where(lane == q, part, whole)
            tiles[g] = whole
            if g == 0:
                table[here] = whole

        def deliver(g):
            for dx in range(NX):
                if g == 0 and dx == 0:
                    continue
                send(tiles.at[g], table.at[here], send_sem.at[2], tile_sem, device(dx=dx, dz=DZ[g]))

        order = program()
        pending = []
        loaded = [None, None]
        partial = [None, None]
        left = [64] * 8
        begun = set()
        ready = []
        chunks = 0

        def pop_one():
            groups, b, c, slot = pending.pop(0)
            for m in range(2):
                g = groups[m]
                value = jnp.max(pltpu.matmul_pop(accs[m][slot]).reshape(ROWS // 8, 8, 2 * E), axis=0)
                left[g] -= 1
                if c == 0:
                    partial[m] = value
                    continue
                value = jnp.maximum(partial[m], value)
                columns = slice(m * TILE, (m + 1) * TILE)
                if (m, g, b) not in begun:
                    begun.add((m, g, b))
                    peaks[g, b, :, columns] = value
                else:
                    value = jnp.maximum(peaks[g, b, :, columns], value)
                    rows[g, pl.ds(row_of[b], 1), columns] = jnp.max(value, axis=0, keepdims=True)
            for g in sorted(set(groups)):
                if left[g] == 0:
                    finish(g)
                    ready.append([2, g])

        def push(m, g):
            pltpu.matmul_push_rhs(
                widened(caps[g, m * TILE : (m + 1) * TILE, :]), staging_register=0, mxu_index=m, transpose=True
            )

        for step in order:
            if step[0] == "c":
                _, slot, t = step
                arrived(cap_part(slot, t), cap_sem.at[slot, t])
                forward_cap(slot, t)
                continue
            if step[0] == "b":
                _, slot, h = step
                arrived(bank_part(slot, h), bank_sem.at[slot, h])
                forward_bank(slot, h)
                continue
            if step[0] == "ready1":
                for dx in (1, NX - 1):
                    pl.semaphore_signal(ready_a, inc=1, device_id=device(dx=dx), device_id_type=MESH)
                continue
            if step[0] == "ready2":
                pl.semaphore_wait(ready_a, 2)
                pl.semaphore_signal(ready_b, inc=1, device_id=device(dx=1), device_id_type=MESH)
                continue
            if step[0] == "ready3":
                pl.semaphore_wait(ready_b, 1)
                continue
            for item in ready:
                item[0] -= 1
            while ready and ready[0][0] < 0:
                deliver(ready.pop(0)[1])
            groups, b, h = step[1:3], step[3], step[4]
            for c in range(HALF // ROWS):
                first = h * HALF + c * ROWS
                lhs = widened(bank[b, first : first + ROWS, :])
                slot = chunks % 4
                chunks += 1
                for m in range(2):
                    fresh = loaded[m] != groups[m]
                    if fresh:
                        push(m, groups[m])
                        loaded[m] = groups[m]
                    pltpu.matmul_acc_lhs(accs[m][slot], lhs, load_staged_rhs=0 if fresh else None)
                pending.append((groups, b, c, slot))
                if len(pending) > 2:
                    pop_one()
        while pending:
            pop_one()
        while ready:
            deliver(ready.pop(0)[1])

        arrived(table.at[pl.ds(0, NX * NZ - 1)], tile_sem)
        arrived(caps.at[pl.ds(0, 7)], send_sem.at[0])
        arrived(bank.at[pl.ds(0, 7)], send_sem.at[1])
        arrived(table.at[pl.ds(0, NX * NZ - 1)], send_sem.at[2])

    pl.run_scoped(
        body,
        *[pltpu.ACC(0)((ROWS, 2 * E), jnp.float32)] * 4,
        *[pltpu.ACC(1)((ROWS, 2 * E), jnp.float32)] * 4,
    )


def ending(table, out_ref, peak_ref, turned):
    x = lax.axis_index("items")
    best = jnp.max(jnp.max(table[...], axis=0), axis=0, keepdims=True)
    mine = table[pl.ds(x * NZ, NZ)].reshape(NZ * 8, 128)
    both = jnp.concatenate([mine - best, jnp.broadcast_to(best, (128 - NZ * 8, 128))], axis=0)
    turned[...] = both.T
    by_user = jnp.concatenate([turned[pl.ds(q, USERS // 4, stride=K), :] for q in range(4)], axis=0)
    out_ref[...] = by_user[:, : NZ * 8]
    square = jnp.concatenate([by_user, by_user], axis=0).T
    peak_ref[...] = square[NZ * 8, :USERS]


def per_device(capsules, bank):
    dma = pltpu.SemaphoreType.DMA
    vmem = pl.BlockSpec(memory_space=pltpu.VMEM)
    table = pl.pallas_call(
        kernel,
        out_shape=jax.ShapeDtypeStruct((NX * NZ, 8, 128), jnp.float32),
        in_specs=[pl.BlockSpec(memory_space=pltpu.HBM)] * 2,
        out_specs=vmem,
        scratch_shapes=[
            pltpu.VMEM((8, COLS, E), jnp.bfloat16),
            pltpu.VMEM((8, BLOCK, E), jnp.bfloat16),
            pltpu.VMEM((8, 8, 8, COLS), jnp.float32),
            pltpu.VMEM((8, 8, COLS), jnp.float32),
            pltpu.VMEM((8, 8, 128), jnp.float32),
            dma((4,)), dma((8, 2)), dma((8, 2)), dma, dma((3,)),
            pltpu.SemaphoreType.REGULAR, pltpu.SemaphoreType.REGULAR,
        ],
        compiler_params=pltpu.CompilerParams(
            collective_id=0, has_side_effects=True, vmem_limit_bytes=40 << 20
        ),
        name="peaks",
    )(
        pltpu.with_memory_space_constraint(capsules.reshape(COLS, E), pltpu.HBM),
        pltpu.with_memory_space_constraint(bank, pltpu.HBM),
    )
    return pl.pallas_call(
        ending,
        out_shape=(
            jax.ShapeDtypeStruct((USERS, NZ * 8), jnp.float32),
            jax.ShapeDtypeStruct((USERS,), jnp.float32),
        ),
        in_specs=[vmem],
        out_specs=(vmem, vmem),
        scratch_shapes=[pltpu.VMEM((128, 128), jnp.float32)],
        compiler_params=pltpu.CompilerParams(vmem_limit_bytes=4 << 20),
        name="ending",
    )(table)


def solution(mesh):
    return jax.shard_map(
        per_device,
        mesh=mesh,
        in_specs=(P("users", None, None), P(("items", "users"), None)),
        out_specs=(P("users", "items"), P("users")),
        check_vma=False,
    )
```

```python
import jax
import jax.numpy as jnp
from jax import lax
from jax.experimental import pallas as pl
from jax.experimental.pallas import tpu as pltpu
from jax.sharding import PartitionSpec as P

K = 8
E = 128
BLOCK = 1024
USERS = 64
NX, NZ, NY = 4, 8, 4
COLS = USERS * K
TILE = COLS // 2
HALF = BLOCK // 2
ROWS = 256
MESH = pl.DeviceIdType.MESH

DZ = (0, -1, -2, -3, 1, 2, 3, 4)
DY = (0, -1, 1, 2)


def units_of(pairs, blocks):
    return [("u", *pair, b, h) for pair in pairs for b, h in blocks]


def full(*slots):
    return [(b, h) for b in slots for h in (0, 1)]


def half(h, *slots):
    return [(b, h) for b in slots]


def wait_c(*pieces):
    return [("c", s, t) for s, t in pieces]


def wait_b(*pieces):
    return [("b", s, h) for s, h in pieces]


def program():
    own, low, high, opposite = (0, 0), [(1, 4), (2, 5), (3, 6)], [(4, 1), (5, 2), (6, 3)], (7, 7)
    order = []
    order += units_of([own], full(0))
    order += wait_b((4, 0), (4, 1))
    order += units_of([own], full(4))
    order += wait_c((1, 0), (4, 1))
    order += units_of([low[0]], full(0, 4))
    order += wait_c((1, 1), (4, 0))
    order += units_of([high[0]], full(0, 4))
    order += wait_b((1, 0), (2, 0))
    order += units_of([own, low[0], high[0]], half(0, 1, 2))
    order += wait_b((5, 0), (6, 0))
    order += units_of([high[0], low[0]], half(0, 5, 6))
    order += wait_c((2, 0), (5, 1))
    order += units_of([own], half(0, 5, 6))
    order += units_of([low[1]], full(0, 4) + half(0, 1, 2))
    order += wait_c((2, 1), (5, 0)) + wait_b((1, 1), (2, 1))
    order += units_of([low[1]], half(0, 5, 6))
    order += units_of([high[1]], full(0, 4) + half(0, 1, 2, 5, 6))
    order += wait_b((5, 1), (6, 1))
    order += units_of([high[1], low[1], low[0]], half(1, 1, 2, 5, 6))
    order += wait_c((3, 0), (6, 1))
    order += units_of([high[0]], half(1, 1, 2, 5, 6))
    order += wait_b((3, 0), (3, 1))
    order += units_of([low[2]], full(0, 4))
    order += wait_c((3, 1), (6, 0)) + [("ready1",)]
    order += units_of([low[2]], full(1, 2, 5, 6))
    order += wait_b((7, 0), (7, 1))
    order += units_of([high[2]], full(0, 4, 1, 2))
    order += [("ready2",)] + wait_c((7, 0), (7, 1))
    order += units_of([high[2]], full(5, 6))
    order += units_of([opposite], full(0, 4, 1, 2))
    order += [("ready3",)]
    order += units_of([opposite], full(5, 6))
    order += units_of([(g, g) for g in (7, 6, 5, 4, 3, 2, 1)], full(3, 7))
    order += units_of([own], half(1, 1, 2, 5, 6) + full(3, 7))
    assert len({o for o in order if o[0] == "u"}) == 128
    return order


def widened(value):
    return jnp.concatenate([value, jnp.zeros_like(value)], axis=1)


def kernel(
    caps_hbm, bank_hbm, table,
    caps, bank, peaks, rows, tiles,
    local_sem, cap_sem, bank_sem, tile_sem, send_sem, ready_a, ready_b,
):
    x = lax.axis_index("items")
    u = lax.axis_index("users")
    z = lax.div(u, 2 * NY)
    y = lax.rem(lax.div(u, 2), NY)
    core = lax.rem(u, 2)
    xs = [lax.rem(x + dx, NX) for dx in range(NX)]
    ys = [lax.rem(y + dy, NY) for dy in range(NY)]
    zs = [lax.rem(z + dz, NZ) for dz in range(NZ)]
    here = x * NZ + z
    users_at = {}
    for dz in range(NZ):
        users_at[dz, 0, 0] = (zs[dz] * NY + y) * 2 + core
    for dy in range(1, NY):
        users_at[0, dy, 0] = (z * NY + ys[dy]) * 2 + core
    users_at[0, 0, 1] = (z * NY + y) * 2 + 1 - core
    row_of = [2 * ys[DY[b % 4] % NY] + (core if b < 4 else 1 - core) for b in range(8)]

    def device(dx=0, dz=0, dy=0, flip=0):
        return {"items": xs[dx % NX], "users": users_at[dz % NZ, dy % NY, flip]}

    def cap_part(slot, t):
        return caps.at[slot, pl.ds(t * TILE, TILE), :]

    def bank_part(slot, h):
        return bank.at[slot, pl.ds(h * HALF, HALF), :]

    def send(src, dst, send_sem, recv_sem, to):
        pltpu.make_async_remote_copy(
            src_ref=src, dst_ref=dst, send_sem=send_sem, recv_sem=recv_sem, device_id=to, device_id_type=MESH
        ).start()

    def send_cap(slot, t, to_slot, dz):
        send(cap_part(slot, t), cap_part(to_slot, t), send_sem.at[0], cap_sem.at[to_slot, t], device(dz=dz))

    def send_bank(slot, h, to_slot, **to):
        send(bank_part(slot, h), bank_part(to_slot, h), send_sem.at[1], bank_sem.at[to_slot, h], device(**to))

    def forward_cap(slot, t):
        if slot in (1, 2):
            send_cap(slot, t, slot + 1, 1)
        elif slot == 3 and t == 0:
            send_cap(3, 0, 7, 1)
        elif slot in (4, 5):
            send_cap(slot, t, slot + 1, -1)
        elif slot == 6 and t == 1:
            send_cap(6, 1, 7, -1)

    def forward_bank(slot, h):
        if slot == 1 and h == 0:
            send_bank(1, 0, 3, dy=1)
        if slot == 2 and h == 1:
            send_bank(2, 1, 3, dy=-1)
        if slot < 4:
            send_bank(slot, h, slot + 4, flip=1)

    def arrived(ref, sem):
        pltpu.make_async_copy(ref, ref, sem).wait()

    def body(*accs):
        accs = (accs[:4], accs[4:])
        own = []
        for t in range(2):
            own.append(pltpu.make_async_copy(caps_hbm.at[pl.ds(t * TILE, TILE), :], cap_part(0, t), local_sem.at[t]))
        for h in range(2):
            own.append(pltpu.make_async_copy(bank_hbm.at[pl.ds(h * HALF, HALF), :], bank_part(0, h), local_sem.at[2 + h]))
        for copy in own:
            copy.start()

        barrier = pltpu.get_barrier_semaphore()
        neighbours = [
            device(flip=1), device(dz=1), device(dz=-1), device(dy=1), device(dy=-1), device(dx=1), device(dx=NX - 1),
        ]
        for neighbour in neighbours:
            pl.semaphore_signal(barrier, inc=1, device_id=neighbour, device_id_type=MESH)

        nothing = jnp.zeros((ROWS, 2 * E), jnp.bfloat16)
        for m in range(2):
            pltpu.matmul_acc_lhs(accs[m][3], nothing, load_staged_rhs=0)
        for m in range(2):
            for acc in accs[m]:
                pltpu.matmul_pop(acc)

        pl.semaphore_wait(barrier, len(neighbours))
        for t in range(2):
            own[t].wait()
        send_cap(0, 0, 1, 1)
        send_cap(0, 1, 4, -1)
        send_cap(0, 1, 1, 1)
        send_cap(0, 0, 4, -1)
        for h in range(2):
            own[2 + h].wait()
            send_bank(0, h, 4, flip=1)
            send_bank(0, h, 1, dy=1)
            send_bank(0, h, 2, dy=-1)

        lane = lax.broadcasted_iota(jnp.int32, (8, 128), 1) % K

        def finish(g):
            whole = None
            for q in range(4):
                part = rows[g, :, q * 128 : (q + 1) * 128]
                for shift in (1, 2, 4):
                    part = jnp.maximum(part, pltpu.roll(part, 128 - shift, 1))
                if q:
                    part = pltpu.roll(part, q, 1)
                whole = part if whole is None else jnp.where(lane == q, part, whole)
            tiles[g] = whole
            if g == 0:
                table[here] = whole

        def deliver(g):
            for dx in (2, 1, 3, 0):
                if g == 0 and dx == 0:
                    continue
                send(tiles.at[g], table.at[here], send_sem.at[2], tile_sem, device(dx=dx, dz=DZ[g]))

        order = program()
        pending = []
        loaded = [None, None]
        partial = [None, None]
        left = [64] * 8
        begun = set()
        ready = []
        chunks = 0

        def pop_one():
            groups, b, c, slot = pending.pop(0)
            for m in range(2):
                g = groups[m]
                value = jnp.max(pltpu.matmul_pop(accs[m][slot]).reshape(ROWS // 8, 8, 2 * E), axis=0)
                left[g] -= 1
                if c == 0:
                    partial[m] = value
                    continue
                value = jnp.maximum(partial[m], value)
                columns = slice(m * TILE, (m + 1) * TILE)
                if (m, g, b) not in begun:
                    begun.add((m, g, b))
                    peaks[g, b, :, columns] = value
                else:
                    value = jnp.maximum(peaks[g, b, :, columns], value)
                    rows[g, pl.ds(row_of[b], 1), columns] = jnp.max(value, axis=0, keepdims=True)
            for g in sorted(set(groups)):
                if left[g] == 0:
                    finish(g)
                    ready.append([2, g])

        def push(m, g):
            pltpu.matmul_push_rhs(
                widened(caps[g, m * TILE : (m + 1) * TILE, :]), staging_register=0, mxu_index=m, transpose=True
            )

        for step in order:
            if step[0] == "c":
                _, slot, t = step
                arrived(cap_part(slot, t), cap_sem.at[slot, t])
                forward_cap(slot, t)
                continue
            if step[0] == "b":
                _, slot, h = step
                arrived(bank_part(slot, h), bank_sem.at[slot, h])
                forward_bank(slot, h)
                continue
            if step[0] == "ready1":
                for dx in (1, NX - 1):
                    pl.semaphore_signal(ready_a, inc=1, device_id=device(dx=dx), device_id_type=MESH)
                continue
            if step[0] == "ready2":
                pl.semaphore_wait(ready_a, 2)
                pl.semaphore_signal(ready_b, inc=1, device_id=device(dx=1), device_id_type=MESH)
                continue
            if step[0] == "ready3":
                pl.semaphore_wait(ready_b, 1)
                continue
            for item in ready:
                item[0] -= 1
            while ready and ready[0][0] < 0:
                deliver(ready.pop(0)[1])
            groups, b, h = step[1:3], step[3], step[4]
            for c in range(HALF // ROWS):
                first = h * HALF + c * ROWS
                lhs = widened(bank[b, first : first + ROWS, :])
                slot = chunks % 4
                chunks += 1
                for m in range(2):
                    fresh = loaded[m] != groups[m]
                    if fresh:
                        push(m, groups[m])
                        loaded[m] = groups[m]
                    pltpu.matmul_acc_lhs(accs[m][slot], lhs, load_staged_rhs=0 if fresh else None)
                pending.append((groups, b, c, slot))
                if len(pending) > 2:
                    pop_one()
        while pending:
            pop_one()
        while ready:
            deliver(ready.pop(0)[1])

        arrived(table.at[pl.ds(0, NX * NZ - 1)], tile_sem)
        arrived(caps.at[pl.ds(0, 7)], send_sem.at[0])
        arrived(bank.at[pl.ds(0, 7)], send_sem.at[1])
        arrived(table.at[pl.ds(0, NX * NZ - 1)], send_sem.at[2])

    pl.run_scoped(
        body,
        *[pltpu.ACC(0)((ROWS, 2 * E), jnp.float32)] * 4,
        *[pltpu.ACC(1)((ROWS, 2 * E), jnp.float32)] * 4,
    )


def ending(table, out_ref, peak_ref, turned):
    x = lax.axis_index("items")
    best = jnp.max(jnp.max(table[...], axis=0), axis=0, keepdims=True)
    mine = table[pl.ds(x * NZ, NZ)].reshape(NZ * 8, 128)
    both = jnp.concatenate([mine - best, jnp.broadcast_to(best, (128 - NZ * 8, 128))], axis=0)
    turned[...] = both.T
    by_user = jnp.concatenate([turned[pl.ds(q, USERS // 4, stride=K), :] for q in range(4)], axis=0)
    out_ref[...] = by_user[:, : NZ * 8]
    square = jnp.concatenate([by_user, by_user], axis=0).T
    peak_ref[...] = square[NZ * 8, :USERS]


def per_device(capsules, bank):
    dma = pltpu.SemaphoreType.DMA
    vmem = pl.BlockSpec(memory_space=pltpu.VMEM)
    table = pl.pallas_call(
        kernel,
        out_shape=jax.ShapeDtypeStruct((NX * NZ, 8, 128), jnp.float32),
        in_specs=[pl.BlockSpec(memory_space=pltpu.HBM)] * 2,
        out_specs=vmem,
        scratch_shapes=[
            pltpu.VMEM((8, COLS, E), jnp.bfloat16),
            pltpu.VMEM((8, BLOCK, E), jnp.bfloat16),
            pltpu.VMEM((8, 8, 8, COLS), jnp.float32),
            pltpu.VMEM((8, 8, COLS), jnp.float32),
            pltpu.VMEM((8, 8, 128), jnp.float32),
            dma((4,)), dma((8, 2)), dma((8, 2)), dma, dma((3,)),
            pltpu.SemaphoreType.REGULAR, pltpu.SemaphoreType.REGULAR,
        ],
        compiler_params=pltpu.CompilerParams(
            collective_id=0, has_side_effects=True, vmem_limit_bytes=40 << 20
        ),
        name="peaks",
    )(
        pltpu.with_memory_space_constraint(capsules.reshape(COLS, E), pltpu.HBM),
        pltpu.with_memory_space_constraint(bank, pltpu.HBM),
    )
    return pl.pallas_call(
        ending,
        out_shape=(
            jax.ShapeDtypeStruct((USERS, NZ * 8), jnp.float32),
            jax.ShapeDtypeStruct((USERS,), jnp.float32),
        ),
        in_specs=[vmem],
        out_specs=(vmem, vmem),
        scratch_shapes=[pltpu.VMEM((128, 128), jnp.float32)],
        compiler_params=pltpu.CompilerParams(vmem_limit_bytes=4 << 20),
        name="ending",
    )(table)


def solution(mesh):
    return jax.shard_map(
        per_device,
        mesh=mesh,
        in_specs=(P("users", None, None), P(("items", "users"), None)),
        out_specs=(P("users", "items"), P("users")),
        check_vma=False,
    )
```

```python
import jax
import jax.numpy as jnp
from jax import lax
from jax.experimental import pallas as pl
from jax.experimental.pallas import tpu as pltpu
from jax.sharding import PartitionSpec as P

K = 8
E = 128
BLOCK = 1024
USERS = 64
NX, NZ, NY = 4, 8, 4
COLS = USERS * K
TILE = COLS // 2
HALF = BLOCK // 2
ROWS = 256
MESH = pl.DeviceIdType.MESH

DZ = (0, -1, -2, -3, 1, 2, 3, 4)
DY = (0, -1, 1, 2)


def units_of(pairs, blocks):
    return [("u", *pair, b, h) for pair in pairs for b, h in blocks]


def full(*slots):
    return [(b, h) for b in slots for h in (0, 1)]


def half(h, *slots):
    return [(b, h) for b in slots]


def wait_c(*pieces):
    return [("c", s, t) for s, t in pieces]


def wait_b(*pieces):
    return [("b", s, h) for s, h in pieces]


def program():
    own, low, high, opposite = (0, 0), [(1, 4), (2, 5), (3, 6)], [(4, 1), (5, 2), (6, 3)], (7, 7)
    order = []
    order += units_of([own], full(0))
    order += wait_b((4, 0), (4, 1))
    order += units_of([own], full(4))
    order += wait_c((1, 0), (4, 1))
    order += units_of([low[0]], full(0, 4))
    order += wait_c((1, 1), (4, 0))
    order += units_of([high[0]], full(0, 4))
    order += wait_b((1, 0), (2, 0))
    order += units_of([own, low[0], high[0]], half(0, 1, 2))
    order += wait_b((5, 0), (6, 0))
    order += units_of([high[0], low[0]], half(0, 5, 6))
    order += wait_c((2, 0), (5, 1))
    order += units_of([low[1]], full(0, 4) + half(0, 1, 2))
    order += wait_c((2, 1), (5, 0)) + wait_b((1, 1), (2, 1))
    order += units_of([low[1]], half(0, 5, 6))
    order += units_of([high[1]], full(0, 4) + half(0, 1, 2, 5, 6))
    order += wait_b((5, 1), (6, 1))
    order += units_of([high[1], low[1], low[0]], half(1, 1, 2, 5, 6))
    order += wait_c((3, 0), (6, 1))
    order += units_of([high[0]], half(1, 1, 2, 5, 6))
    order += wait_b((3, 0), (3, 1))
    order += units_of([low[2]], full(0, 4))
    order += wait_c((3, 1), (6, 0)) + [("ready1",)]
    order += units_of([low[2]], full(1, 2, 5, 6))
    order += wait_b((7, 0), (7, 1))
    order += units_of([high[2]], full(0, 4, 1, 2))
    order += [("ready2",)] + wait_c((7, 0), (7, 1))
    order += units_of([high[2]], full(5, 6))
    order += units_of([opposite], full(0, 4, 1, 2))
    order += [("ready3",)]
    order += units_of([opposite], full(5, 6))
    order += units_of([(g, g) for g in (7, 6, 5, 4, 3, 2, 1)], full(3, 7))
    order += units_of([own], half(0, 5, 6) + half(1, 1, 2, 5, 6) + full(3, 7))
    assert len({o for o in order if o[0] == "u"}) == 128
    return order


def widened(value):
    return jnp.concatenate([value, jnp.zeros_like(value)], axis=1)


def kernel(
    caps_hbm, bank_hbm, table,
    caps, bank, peaks, rows, tiles,
    local_sem, cap_sem, bank_sem, tile_sem, send_sem, ready_a, ready_b,
):
    x = lax.axis_index("items")
    u = lax.axis_index("users")
    z = lax.div(u, 2 * NY)
    y = lax.rem(lax.div(u, 2), NY)
    core = lax.rem(u, 2)
    xs = [lax.rem(x + dx, NX) for dx in range(NX)]
    ys = [lax.rem(y + dy, NY) for dy in range(NY)]
    zs = [lax.rem(z + dz, NZ) for dz in range(NZ)]
    here = x * NZ + z
    users_at = {}
    for dz in range(NZ):
        users_at[dz, 0, 0] = (zs[dz] * NY + y) * 2 + core
    for dy in range(1, NY):
        users_at[0, dy, 0] = (z * NY + ys[dy]) * 2 + core
    users_at[0, 0, 1] = (z * NY + y) * 2 + 1 - core
    row_of = [2 * ys[DY[b % 4] % NY] + (core if b < 4 else 1 - core) for b in range(8)]

    def device(dx=0, dz=0, dy=0, flip=0):
        return {"items": xs[dx % NX], "users": users_at[dz % NZ, dy % NY, flip]}

    def cap_part(slot, t):
        return caps.at[slot, pl.ds(t * TILE, TILE), :]

    def bank_part(slot, h):
        return bank.at[slot, pl.ds(h * HALF, HALF), :]

    def send(src, dst, send_sem, recv_sem, to):
        pltpu.make_async_remote_copy(
            src_ref=src, dst_ref=dst, send_sem=send_sem, recv_sem=recv_sem, device_id=to, device_id_type=MESH
        ).start()

    def send_cap(slot, t, to_slot, dz):
        send(cap_part(slot, t), cap_part(to_slot, t), send_sem.at[0], cap_sem.at[to_slot, t], device(dz=dz))

    def send_bank(slot, h, to_slot, **to):
        send(bank_part(slot, h), bank_part(to_slot, h), send_sem.at[1], bank_sem.at[to_slot, h], device(**to))

    def forward_cap(slot, t):
        if slot in (1, 2):
            send_cap(slot, t, slot + 1, 1)
        elif slot == 3 and t == 0:
            send_cap(3, 0, 7, 1)
        elif slot in (4, 5):
            send_cap(slot, t, slot + 1, -1)
        elif slot == 6 and t == 1:
            send_cap(6, 1, 7, -1)

    def forward_bank(slot, h):
        if slot == 1 and h == 0:
            send_bank(1, 0, 3, dy=1)
        if slot == 2 and h == 1:
            send_bank(2, 1, 3, dy=-1)
        if slot < 4:
            send_bank(slot, h, slot + 4, flip=1)

    def arrived(ref, sem):
        pltpu.make_async_copy(ref, ref, sem).wait()

    def body(*accs):
        accs = (accs[:4], accs[4:])
        own = []
        for t in range(2):
            own.append(pltpu.make_async_copy(caps_hbm.at[pl.ds(t * TILE, TILE), :], cap_part(0, t), local_sem.at[t]))
        for h in range(2):
            own.append(pltpu.make_async_copy(bank_hbm.at[pl.ds(h * HALF, HALF), :], bank_part(0, h), local_sem.at[2 + h]))
        for copy in own:
            copy.start()

        barrier = pltpu.get_barrier_semaphore()
        neighbours = [
            device(flip=1), device(dz=1), device(dz=-1), device(dy=1), device(dy=-1), device(dx=1), device(dx=NX - 1),
        ]
        for neighbour in neighbours:
            pl.semaphore_signal(barrier, inc=1, device_id=neighbour, device_id_type=MESH)

        nothing = jnp.zeros((ROWS, 2 * E), jnp.bfloat16)
        for m in range(2):
            pltpu.matmul_acc_lhs(accs[m][3], nothing, load_staged_rhs=0)
        for m in range(2):
            for acc in accs[m]:
                pltpu.matmul_pop(acc)

        pl.semaphore_wait(barrier, len(neighbours))
        for t in range(2):
            own[t].wait()
        send_cap(0, 0, 1, 1)
        send_cap(0, 1, 4, -1)
        send_cap(0, 1, 1, 1)
        send_cap(0, 0, 4, -1)
        for h in range(2):
            own[2 + h].wait()
            send_bank(0, h, 4, flip=1)
            send_bank(0, h, 1, dy=1)
            send_bank(0, h, 2, dy=-1)

        lane = lax.broadcasted_iota(jnp.int32, (8, 128), 1) % K

        def finish(g):
            whole = None
            for q in range(4):
                part = rows[g, :, q * 128 : (q + 1) * 128]
                for shift in (1, 2, 4):
                    part = jnp.maximum(part, pltpu.roll(part, 128 - shift, 1))
                if q:
                    part = pltpu.roll(part, q, 1)
                whole = part if whole is None else jnp.where(lane == q, part, whole)
            tiles[g] = whole
            if g == 0:
                table[here] = whole

        def deliver(g):
            for dx in (2, 1, 3, 0):
                if g == 0 and dx == 0:
                    continue
                send(tiles.at[g], table.at[here], send_sem.at[2], tile_sem, device(dx=dx, dz=DZ[g]))

        order = program()
        pending = []
        loaded = [None, None]
        partial = [None, None]
        left = [64] * 8
        begun = set()
        ready = []
        chunks = 0

        def pop_one():
            groups, b, c, slot = pending.pop(0)
            for m in range(2):
                g = groups[m]
                value = jnp.max(pltpu.matmul_pop(accs[m][slot]).reshape(ROWS // 8, 8, 2 * E), axis=0)
                left[g] -= 1
                if c == 0:
                    partial[m] = value
                    continue
                value = jnp.maximum(partial[m], value)
                columns = slice(m * TILE, (m + 1) * TILE)
                if (m, g, b) not in begun:
                    begun.add((m, g, b))
                    peaks[g, b, :, columns] = value
                else:
                    value = jnp.maximum(peaks[g, b, :, columns], value)
                    rows[g, pl.ds(row_of[b], 1), columns] = jnp.max(value, axis=0, keepdims=True)
            for g in sorted(set(groups)):
                if left[g] == 0:
                    finish(g)
                    ready.append([2, g])

        def push(m, g):
            pltpu.matmul_push_rhs(
                widened(caps[g, m * TILE : (m + 1) * TILE, :]), staging_register=0, mxu_index=m, transpose=True
            )

        for step in order:
            if step[0] == "c":
                _, slot, t = step
                arrived(cap_part(slot, t), cap_sem.at[slot, t])
                forward_cap(slot, t)
                continue
            if step[0] == "b":
                _, slot, h = step
                arrived(bank_part(slot, h), bank_sem.at[slot, h])
                forward_bank(slot, h)
                continue
            if step[0] == "ready1":
                for dx in (1, NX - 1):
                    pl.semaphore_signal(ready_a, inc=1, device_id=device(dx=dx), device_id_type=MESH)
                continue
            if step[0] == "ready2":
                pl.semaphore_wait(ready_a, 2)
                pl.semaphore_signal(ready_b, inc=1, device_id=device(dx=1), device_id_type=MESH)
                continue
            if step[0] == "ready3":
                pl.semaphore_wait(ready_b, 1)
                continue
            for item in ready:
                item[0] -= 1
            while ready and ready[0][0] < 0:
                deliver(ready.pop(0)[1])
            groups, b, h = step[1:3], step[3], step[4]
            for c in range(HALF // ROWS):
                first = h * HALF + c * ROWS
                lhs = widened(bank[b, first : first + ROWS, :])
                slot = chunks % 4
                chunks += 1
                for m in range(2):
                    fresh = loaded[m] != groups[m]
                    if fresh:
                        push(m, groups[m])
                        loaded[m] = groups[m]
                    pltpu.matmul_acc_lhs(accs[m][slot], lhs, load_staged_rhs=0 if fresh else None)
                pending.append((groups, b, c, slot))
                if len(pending) > 2:
                    pop_one()
        while pending:
            pop_one()
        while ready:
            deliver(ready.pop(0)[1])

        arrived(table.at[pl.ds(0, NX * NZ - 1)], tile_sem)
        arrived(caps.at[pl.ds(0, 7)], send_sem.at[0])
        arrived(bank.at[pl.ds(0, 7)], send_sem.at[1])
        arrived(table.at[pl.ds(0, NX * NZ - 1)], send_sem.at[2])

    pl.run_scoped(
        body,
        *[pltpu.ACC(0)((ROWS, 2 * E), jnp.float32)] * 4,
        *[pltpu.ACC(1)((ROWS, 2 * E), jnp.float32)] * 4,
    )


def ending(table, out_ref, peak_ref, turned):
    x = lax.axis_index("items")
    best = jnp.max(jnp.max(table[...], axis=0), axis=0, keepdims=True)
    mine = table[pl.ds(x * NZ, NZ)].reshape(NZ * 8, 128)
    both = jnp.concatenate([mine - best, jnp.broadcast_to(best, (128 - NZ * 8, 128))], axis=0)
    turned[...] = both.T
    by_user = jnp.concatenate([turned[pl.ds(q, USERS // 4, stride=K), :] for q in range(4)], axis=0)
    out_ref[...] = by_user[:, : NZ * 8]
    square = jnp.concatenate([by_user, by_user], axis=0).T
    peak_ref[...] = square[NZ * 8, :USERS]


def per_device(capsules, bank):
    dma = pltpu.SemaphoreType.DMA
    vmem = pl.BlockSpec(memory_space=pltpu.VMEM)
    table = pl.pallas_call(
        kernel,
        out_shape=jax.ShapeDtypeStruct((NX * NZ, 8, 128), jnp.float32),
        in_specs=[pl.BlockSpec(memory_space=pltpu.HBM)] * 2,
        out_specs=vmem,
        scratch_shapes=[
            pltpu.VMEM((8, COLS, E), jnp.bfloat16),
            pltpu.VMEM((8, BLOCK, E), jnp.bfloat16),
            pltpu.VMEM((8, 8, 8, COLS), jnp.float32),
            pltpu.VMEM((8, 8, COLS), jnp.float32),
            pltpu.VMEM((8, 8, 128), jnp.float32),
            dma((4,)), dma((8, 2)), dma((8, 2)), dma, dma((3,)),
            pltpu.SemaphoreType.REGULAR, pltpu.SemaphoreType.REGULAR,
        ],
        compiler_params=pltpu.CompilerParams(
            collective_id=0, has_side_effects=True, vmem_limit_bytes=40 << 20
        ),
        name="peaks",
    )(
        pltpu.with_memory_space_constraint(capsules.reshape(COLS, E), pltpu.HBM),
        pltpu.with_memory_space_constraint(bank, pltpu.HBM),
    )
    return pl.pallas_call(
        ending,
        out_shape=(
            jax.ShapeDtypeStruct((USERS, NZ * 8), jnp.float32),
            jax.ShapeDtypeStruct((USERS,), jnp.float32),
        ),
        in_specs=[vmem],
        out_specs=(vmem, vmem),
        scratch_shapes=[pltpu.VMEM((128, 128), jnp.float32)],
        compiler_params=pltpu.CompilerParams(vmem_limit_bytes=4 << 20),
        name="ending",
    )(table)


def solution(mesh):
    return jax.shard_map(
        per_device,
        mesh=mesh,
        in_specs=(P("users", None, None), P(("items", "users"), None)),
        out_specs=(P("users", "items"), P("users")),
        check_vma=False,
    )
```
